32 devices in a mesh: grp: 1, tile: 16 (over z, x, core), mem: 2 (over y).
Axes of the slice: x: 2, y: 2, z: 4, core: 2. Of those that a mesh axis runs over, the one named last changes fastest.
Arguments:
- ens_coarse: bfloat16 [1, 80, 128, 64, 64], P('grp', 'mem', None, 'tile'), may hold values from -6 to 6
- col_interp: bfloat16 [128, 64], replicated, may hold values from -0.75 to 0.75
- row_weights: bfloat16 [3, 128], replicated, may hold values from 0.099609375 to 0.8984375
- ctrl_vec: float32 [1, 128, 128, 128], P('grp', None, 'tile'), may hold values from -24 to 24
- band_loc: bfloat16 [128, 24], P('tile'), may hold values from -1.25 to 1.25
- row_loc: bfloat16 [128, 128], replicated, may hold values from -0.5 to 0.5
- level_loc: bfloat16 [128, 128], replicated, may hold values from -0.5 to 0.5
- hx_pert: bfloat16 [1, 80, 65536], P('grp', None, ('tile', 'mem')), may hold values from -3 to 3
- innov: float32 [1, 65536], P('grp', ('tile', 'mem')), may hold values from -48 to 48
- obs_prec: float32 [1, 65536], P('grp', ('tile', 'mem')), may hold values from 0.3 to 3
- obs_region: int32 [1, 65536], P('grp', ('tile', 'mem')), may hold values from 0 to 7
Outputs:
- increment: float32 [1, 128, 128, 128], P('grp', 'mem', 'tile')
- letkf_weights: float32 [128, 80], P('tile')
The draws below stay inside these ranges and needn't reach their ends.
Inputs may be any that keep to these rules, and one draw needn't show every extreme that they name: `obs_region`: the region of an observation among the 8 regions of its block of 4096 observations.
All inputs are finite; a program needn't handle non-finite values.
Results may differ from the reference program's by a relative error of at most 0.018.
Values may be sent and summed in bfloat16 or wider, within the bound.
A program may use at most 128 MiB of HBM per device.

```python
import math
import jax
import jax.numpy as jnp
from jax import lax

MEMBERS = 80
LEV = 128
NREG = 8
FCD = 8
TSLOTS = 1
CR = 64
FR = 128
FC = 128
CC = 64
NOBS = 65536
N_TILE = 16


def place_ends(drawn, own_key, low, largest):
    spot = [jax.random.randint(jax.random.fold_in(own_key, axis), (), 0, length) for axis, length in enumerate(drawn.shape)]
    widest = drawn.shape.index(max(drawn.shape))
    neighbour = spot[:widest] + [(spot[widest] + 1) % drawn.shape[widest]] + spot[widest + 1:]
    return drawn.at[tuple(spot)].set(low).at[tuple(neighbour)].set(largest)


def level_of(rng, extent, split, least, high):
    level = 1.0
    for dim, shards_of in split:
        draws = jax.random.uniform(jax.random.fold_in(jax.random.fold_in(rng, 6), dim), (shards_of,), jnp.float32, least / len(split), high / len(split))
        level = level * jnp.repeat(jnp.exp(draws), extent[dim] // shards_of).reshape((-1,) + (1,) * (len(extent) - 1 - dim))
    return level


def noise(stream_key, extent, width, limit, pieces=(), kind=jnp.bfloat16):
    values = width * jax.random.normal(stream_key, extent, jnp.float32)
    if pieces:
        values = values * level_of(stream_key, extent, pieces, -0.22, 0.18)
    return jnp.clip(values, -limit, limit).astype(kind)


def setup_inputs(seed: int = 0) -> dict:
    arg_keys = jax.random.split(jax.random.key(seed), 12)
    return {
        "ens_coarse": noise(arg_keys[0], (TSLOTS, MEMBERS, LEV, CR, CC), 1.0, 6.0, ((1, 2), (3, 16))),
        "col_interp": noise(arg_keys[1], (FC, CC), CC ** -0.5, 0.75),
        "row_weights": jnp.clip(jax.random.uniform(arg_keys[2], (3, FR), jnp.float32, 0.099609375, 0.8984375), 0.099609375, 0.8984375).astype(jnp.bfloat16),
        "ctrl_vec": noise(arg_keys[3], (TSLOTS, LEV, FC, FR), 4.0, 24.0, ((2, 16),), jnp.float32),
        "band_loc": noise(arg_keys[4], (FC, 3 * FCD), (3 * FCD) ** -0.5, 1.25, ((0, 16),)),
        "row_loc": noise(arg_keys[5], (FR, FR), FR ** -0.5, 0.5),
        "level_loc": noise(arg_keys[6], (LEV, LEV), LEV ** -0.5, 0.5),
        "hx_pert": noise(arg_keys[7], (TSLOTS, MEMBERS, NOBS), 0.5, 3.0, ((2, 32),)),
        "innov": noise(arg_keys[8], (TSLOTS, NOBS), 8.0, 48.0, ((1, 32),), jnp.float32),
        "obs_prec": jnp.clip(jnp.exp(math.log(3.0) - 2.3025851 * jax.random.uniform(arg_keys[9], (TSLOTS, NOBS), jnp.float32) ** level_of(arg_keys[9], (TSLOTS, NOBS), ((1, 32),), -0.2, 0.2)), 0.3, 3.0),
        "obs_region": place_ends(jax.random.randint(arg_keys[10], (TSLOTS, NOBS), 0, NREG), jax.random.fold_in(arg_keys[10], 1), 0, NREG - 1).astype(jnp.int32),
    }


def to_half(value):
    return lax.optimization_barrier(value.astype(jnp.bfloat16))

def solve_weights(gram_sums, right_side):
    member_count = gram_sums.shape[-1]
    system = gram_sums + (member_count - 1) * jnp.eye(member_count, dtype=jnp.float32)
    factor = jnp.linalg.cholesky(system)
    halfway = lax.linalg.triangular_solve(factor, right_side[..., None], left_side=True, lower=True)
    result = lax.linalg.triangular_solve(factor, halfway, left_side=True, lower=True, transpose_a=True)
    return result[..., 0]

def fine_member(ens_member, col_interp, row_weights):
    coarse_cols = jnp.einsum('tlic,jc->tlij', ens_member.astype(jnp.float32), col_interp.astype(jnp.float32), precision=lax.Precision.HIGHEST)
    padded = jnp.pad(to_half(coarse_cols).astype(jnp.float32), ((0, 0), (0, 0), (1, 1), (0, 0)))
    fine_rows = row_weights.shape[1]
    parent_row = jnp.arange(fine_rows, dtype=jnp.int32) // 2
    weights = row_weights.astype(jnp.float32)
    running = jnp.zeros(padded.shape[:2] + (fine_rows, padded.shape[3]), jnp.float32)
    for offset in range(3):
        running = running + weights[offset][None, None, :, None] * jnp.take(padded, parent_row + offset, axis=2)
    return jnp.swapaxes(to_half(running), 2, 3)

def band_apply(projected, band_loc):
    levels, columns_all, rows_all = projected.shape
    band_width = band_loc.shape[1] // 3
    blocks = columns_all // band_width
    padded = jnp.pad(projected.astype(jnp.float32), ((0, 0), (band_width, band_width), (0, 0)))
    window_index = jnp.arange(blocks, dtype=jnp.int32)[:, None] * band_width + jnp.arange(3 * band_width, dtype=jnp.int32)[None, :]
    windows = jnp.take(padded, window_index, axis=1)
    band_table = band_loc.astype(jnp.float32).reshape(blocks, band_width, 3 * band_width)
    result = jnp.einsum('bjq,lbqr->lbjr', band_table, windows, precision=lax.Precision.HIGHEST)
    return to_half(result.reshape(levels, columns_all, rows_all))

def reference(ens_coarse, col_interp, row_weights, ctrl_vec, band_loc, row_loc, level_loc, hx_pert, innov, obs_prec, obs_region):
    members = ens_coarse.shape[1]
    row_table = row_loc.astype(jnp.float32)
    level_table = level_loc.astype(jnp.float32)

    def one_member(running, ens_member):
        refined = fine_member(ens_member, col_interp, row_weights)
        slot_term = to_half(refined.astype(jnp.float32) * ctrl_vec)
        projected = to_half(jnp.sum(slot_term.astype(jnp.float32), axis=0))
        banded = band_apply(projected, band_loc)
        row_mixed = to_half(jnp.einsum('ljs,rs->ljr', banded.astype(jnp.float32), row_table, precision=lax.Precision.HIGHEST))
        localized = to_half(jnp.einsum('lm,mjr->ljr', level_table, row_mixed.astype(jnp.float32), precision=lax.Precision.HIGHEST))
        return (running + refined.astype(jnp.float32) * localized.astype(jnp.float32)[None], None)
    running, unused = lax.scan(one_member, jnp.zeros(ctrl_vec.shape, jnp.float32), jnp.moveaxis(ens_coarse, 1, 0))
    increment = running / (members - 1)
    tile_count = N_TILE
    obs_tile = hx_pert.shape[2] // tile_count

    def one_tile(tile_index):
        obs_start = tile_index * obs_tile
        observed = lax.dynamic_slice_in_dim(hx_pert, obs_start, obs_tile, 2).astype(jnp.float32)
        precision_row = lax.dynamic_slice_in_dim(obs_prec, obs_start, obs_tile, 1)
        innovation = lax.dynamic_slice_in_dim(innov, obs_start, obs_tile, 1)
        region = lax.dynamic_slice_in_dim(obs_region, obs_start, obs_tile, 1)
        weighted = to_half(observed * precision_row[:, None, :]).astype(jnp.float32)
        labels = jnp.arange(NREG, dtype=jnp.int32)
        member_of = (region[:, None, :] == labels[None, :, None]).astype(jnp.float32)
        gram_sums = jnp.einsum('tko,tro,tjo->rkj', weighted, member_of, observed, precision=lax.Precision.HIGHEST)
        right_side = jnp.einsum('tko,tro,to->rk', weighted, member_of, innovation, precision=lax.Precision.HIGHEST)
        return solve_weights(gram_sums, right_side)
    weights = lax.map(one_tile, jnp.arange(tile_count, dtype=jnp.int32))
    return (increment, weights.reshape(tile_count * NREG, members))
```

```python
import jax
import jax.numpy as jnp
from jax import lax
from jax.sharding import PartitionSpec as P

NREG = 8


def extended(value, sides, width):
    for axis, dim in sides:
        peers, length = (lax.axis_size(axis), value.shape[dim])
        up = [(i, (i + 1) % peers) for i in range(peers - 1)]
        down = [(j, i) for i, j in up]
        last = lax.slice_in_dim(value, length - width, length, axis=dim)
        first = lax.slice_in_dim(value, 0, width, axis=dim)
        before = lax.ppermute(last, axis, up)
        after = lax.ppermute(first, axis, down)
        value = jnp.concatenate([before, value, after], axis=dim)
    return value


def swap_add(value):
    peers = lax.axis_size("mem")
    me = lax.axis_index("mem")
    length = value.shape[0] // peers
    total = lax.dynamic_slice_in_dim(value, me * length, length, 0)
    for shift in range(1, peers):
        other = lax.rem(me + shift, peers)
        part = lax.dynamic_slice_in_dim(value, other * length, length, 0)
        pairs = [(i, (i + shift) % peers) for i in range(peers)]
        total = total + lax.ppermute(part, "mem", pairs)
    return total


def collect(value):
    peers = lax.axis_size("mem")
    me = lax.axis_index("mem")
    length = value.shape[0]
    result = jnp.zeros((peers * length,) + value.shape[1:], value.dtype)
    result = lax.dynamic_update_slice_in_dim(result, value, me * length, 0)
    for shift in range(1, peers):
        pairs = [(i, (i + shift) % peers) for i in range(peers)]
        moved = lax.ppermute(value, "mem", pairs)
        source = lax.rem(me + peers - shift, peers)
        result = lax.dynamic_update_slice_in_dim(result, moved, source * length, 0)
    return result


def row_matrix(row_weights, fine_rows, coarse_rows):
    fine_index = lax.broadcasted_iota(jnp.int32, (fine_rows, coarse_rows), 0)
    coarse_index = lax.broadcasted_iota(jnp.int32, (fine_rows, coarse_rows), 1)
    weights = row_weights.astype(jnp.float32)
    stencil = jnp.zeros((fine_rows, coarse_rows), jnp.float32)
    for offset in range(3):
        matched = coarse_index == fine_index // 2 + offset - 1
        stencil = stencil + jnp.where(matched, weights[offset][:, None], 0.0)
    return stencil.astype(jnp.bfloat16)


def solve_weights(gram_sums, right_side):
    member_count = gram_sums.shape[-1]
    system = gram_sums + (member_count - 1) * jnp.eye(member_count, dtype=jnp.float32)
    factor = jnp.linalg.cholesky(system)
    halfway = lax.linalg.triangular_solve(factor, right_side[..., None], left_side=True, lower=True)
    result = lax.linalg.triangular_solve(
        factor, halfway, left_side=True, lower=True, transpose_a=True
    )
    return result[..., 0]


def body(
    ens_coarse,
    col_interp,
    row_weights,
    ctrl_vec,
    band_loc,
    row_loc,
    level_loc,
    hx_pert,
    innov,
    obs_prec,
    obs_region,
):
    fine_rows = row_weights.shape[1]
    columns = band_loc.shape[0]
    total_members = hx_pert.shape[1]
    observed = hx_pert[0]
    weighted = (observed * obs_prec[0][None, :]).astype(jnp.bfloat16)
    labels = lax.broadcasted_iota(jnp.int32, (NREG, observed.shape[1]), 0)
    member_of = obs_region[0][None, :] == labels
    masked = jnp.where(member_of[:, None, :], weighted[None], jnp.zeros((), jnp.bfloat16))
    gram_sums = jnp.einsum("rko,jo->rkj", masked, observed, preferred_element_type=jnp.float32)
    innov_rows = jnp.where(member_of, innov[0][None, :], 0.0)
    right_side = jnp.dot(
        innov_rows, weighted.astype(jnp.float32).T, precision=lax.Precision.HIGHEST
    )
    sums = jnp.concatenate([gram_sums, right_side[:, :, None]], axis=2)
    sums = swap_add(lax.psum(sums, "grp") if lax.axis_size("grp") > 1 else sums)
    coarse_cols = jnp.einsum(
        "tklic,jc->tklij", ens_coarse, col_interp, preferred_element_type=jnp.float32
    ).astype(jnp.bfloat16)
    stencil = row_matrix(row_weights, fine_rows, fine_rows // 2)
    refined = jnp.einsum(
        "tklij,ri->tkljr",
        lax.all_to_all(coarse_cols, "tile", split_axis=4, concat_axis=3, tiled=True),
        stencil,
        preferred_element_type=jnp.float32,
    ).astype(jnp.bfloat16)
    member_fine = refined[0]
    slot_term = member_fine * ctrl_vec[0][None]
    projected = slot_term.astype(jnp.bfloat16)
    if lax.axis_size("grp") > 1:
        projected = lax.psum(projected, "grp")
    padded = extended(projected, (("tile", 2),), columns)
    banded = jnp.einsum(
        "jq,klqr->kljr", band_loc, padded, preferred_element_type=jnp.float32
    ).astype(jnp.bfloat16)
    row_mixed = jnp.einsum(
        "kljs,rs->kljr", banded, row_loc, preferred_element_type=jnp.float32
    ).astype(jnp.bfloat16)
    localized = jnp.einsum(
        "lm,kmjr->kljr", level_loc, row_mixed, preferred_element_type=jnp.float32
    ).astype(jnp.bfloat16)
    increment = swap_add(
        jnp.sum(member_fine.astype(jnp.float32) * localized.astype(jnp.float32), axis=0)
    ) / (total_members - 1)
    own_weights = solve_weights(sums[:, :, :total_members], sums[:, :, total_members])
    weights = collect(own_weights)
    return (increment[None], weights)


def solution(mesh):
    placed = (
        P("grp", "mem", None, "tile", None),
        P(),
        P(),
        P("grp", None, "tile", None),
        P("tile", None),
        P(),
        P(),
        P("grp", None, ("tile", "mem")),
        P("grp", ("tile", "mem")),
        P("grp", ("tile", "mem")),
        P("grp", ("tile", "mem")),
    )
    return jax.shard_map(
        body,
        mesh=mesh,
        in_specs=placed,
        out_specs=(P("grp", "mem", "tile", None), P("tile", None)),
        check_vma=False,
    )
```

```python
import jax
import jax.numpy as jnp
from jax import lax
from jax.experimental import pallas as pl
from jax.experimental.pallas import tpu as pltpu
from jax.sharding import PartitionSpec as P

NREG = 8
GROUP = 16
CHUNKS = 2


def extended(value, sides, width):
    for axis, dim in sides:
        peers, length = (lax.axis_size(axis), value.shape[dim])
        up = [(i, (i + 1) % peers) for i in range(peers - 1)]
        down = [(j, i) for i, j in up]
        last = lax.slice_in_dim(value, length - width, length, axis=dim)
        first = lax.slice_in_dim(value, 0, width, axis=dim)
        before = lax.ppermute(last, axis, up)
        after = lax.ppermute(first, axis, down)
        value = jnp.concatenate([before, value, after], axis=dim)
    return value


def swap_add(value):
    peers = lax.axis_size("mem")
    me = lax.axis_index("mem")
    length = value.shape[0] // peers
    total = lax.dynamic_slice_in_dim(value, me * length, length, 0)
    for shift in range(1, peers):
        other = lax.rem(me + shift, peers)
        part = lax.dynamic_slice_in_dim(value, other * length, length, 0)
        pairs = [(i, (i + shift) % peers) for i in range(peers)]
        total = total + lax.ppermute(part, "mem", pairs)
    return total


def collect(value):
    peers = lax.axis_size("mem")
    me = lax.axis_index("mem")
    length = value.shape[0]
    result = jnp.zeros((peers * length,) + value.shape[1:], value.dtype)
    result = lax.dynamic_update_slice_in_dim(result, value, me * length, 0)
    for shift in range(1, peers):
        pairs = [(i, (i + shift) % peers) for i in range(peers)]
        moved = lax.ppermute(value, "mem", pairs)
        source = lax.rem(me + peers - shift, peers)
        result = lax.dynamic_update_slice_in_dim(result, moved, source * length, 0)
    return result


def row_matrix(row_weights, fine_rows, coarse_rows):
    fine_index = lax.broadcasted_iota(jnp.int32, (fine_rows, coarse_rows), 0)
    coarse_index = lax.broadcasted_iota(jnp.int32, (fine_rows, coarse_rows), 1)
    weights = row_weights.astype(jnp.float32)
    stencil = jnp.zeros((fine_rows, coarse_rows), jnp.float32)
    for offset in range(3):
        matched = coarse_index == fine_index // 2 + offset - 1
        stencil = stencil + jnp.where(matched, weights[offset][:, None], 0.0)
    return stencil.astype(jnp.bfloat16)


def solve_weights(gram_sums, right_side):
    member_count = gram_sums.shape[-1]
    system = gram_sums + (member_count - 1) * jnp.eye(member_count, dtype=jnp.float32)
    factor = jnp.linalg.cholesky(system)
    halfway = lax.linalg.triangular_solve(factor, right_side[..., None], left_side=True, lower=True)
    result = lax.linalg.triangular_solve(
        factor, halfway, left_side=True, lower=True, transpose_a=True
    )
    return result[..., 0]


def plain_increment(
    ens_coarse, col_interp, row_weights, ctrl_vec, band_loc, row_loc, level_loc, total_members
):
    fine_rows = row_weights.shape[1]
    columns = band_loc.shape[0]
    coarse_cols = jnp.einsum(
        "tklic,jc->tklij", ens_coarse, col_interp, preferred_element_type=jnp.float32
    ).astype(jnp.bfloat16)
    stencil = row_matrix(row_weights, fine_rows, fine_rows // 2)
    refined = jnp.einsum(
        "tklij,ri->tkljr",
        lax.all_to_all(coarse_cols, "tile", split_axis=4, concat_axis=3, tiled=True),
        stencil,
        preferred_element_type=jnp.float32,
    ).astype(jnp.bfloat16)
    member_fine = refined[0]
    slot_term = member_fine * ctrl_vec[0][None]
    projected = slot_term.astype(jnp.bfloat16)
    if lax.axis_size("grp") > 1:
        projected = lax.psum(projected, "grp")
    padded = extended(projected, (("tile", 2),), columns)
    banded = jnp.einsum(
        "jq,klqr->kljr", band_loc, padded, preferred_element_type=jnp.float32
    ).astype(jnp.bfloat16)
    row_mixed = jnp.einsum(
        "kljs,rs->kljr", banded, row_loc, preferred_element_type=jnp.float32
    ).astype(jnp.bfloat16)
    localized = jnp.einsum(
        "lm,kmjr->kljr", level_loc, row_mixed, preferred_element_type=jnp.float32
    ).astype(jnp.bfloat16)
    return swap_add(
        jnp.sum(member_fine.astype(jnp.float32) * localized.astype(jnp.float32), axis=0)
    ) / (total_members - 1)


def member_kernel(
    before, own, after, ctrl, stencil, band, row_loc, level_loc, total, proj, fine, banded, mixed
):
    columns, levels, rows = total.shape
    window = proj.shape[0]

    @pl.when(pl.program_id(0) == 0)
    def _():
        total[...] = jnp.zeros_like(total)

    for q in range(window):
        source = (before, own, after)[q // columns]
        refined = lax.dot_general(
            source[0, q % columns],
            stencil[...],
            (((0,), (0,)), ((), ())),
            preferred_element_type=jnp.float32,
        ).astype(jnp.bfloat16)
        if q // columns == 1:
            fine[q % columns] = refined
        proj[q] = (refined.astype(jnp.float32) * ctrl[q]).astype(jnp.bfloat16)
    for pair in range(levels // (2 * GROUP)):
        parts = []
        for half in range(2):
            start = (2 * pair + half) * GROUP
            parts.append(proj[:, start : start + GROUP, :].reshape(window * GROUP, rows))
        result = jnp.dot(
            band[...], jnp.concatenate(parts, axis=1), preferred_element_type=jnp.float32
        ).astype(jnp.bfloat16)
        for half in range(2):
            start = (2 * pair + half) * GROUP
            banded[:, start : start + GROUP, :] = result[:, half * rows : (half + 1) * rows].reshape(
                columns, GROUP, rows
            )
    mixed[...] = lax.dot_general(
        banded[...].reshape(columns * levels, rows),
        row_loc[...],
        (((1,), (1,)), ((), ())),
        preferred_element_type=jnp.float32,
    ).astype(jnp.bfloat16)
    for j in range(columns):
        localized = jnp.dot(
            level_loc[...],
            mixed[j * levels : (j + 1) * levels, :],
            preferred_element_type=jnp.float32,
        )
        total[j] += fine[j].astype(jnp.float32) * localized


def member_sum(before, own, after, ctrl, stencil, band, row_loc, level_loc):
    members, columns, coarse_rows, levels = own.shape
    window, _, rows = ctrl.shape
    block = pl.BlockSpec((1, columns, coarse_rows, levels), lambda k: (k, 0, 0, 0))

    def whole(value):
        return pl.BlockSpec(value.shape, lambda k: (0,) * value.ndim)

    flops = 2 * members * levels * rows * (
        window * coarse_rows + columns * (window * GROUP + rows + levels)
    )
    return pl.pallas_call(
        member_kernel,
        grid=(members,),
        out_shape=jax.ShapeDtypeStruct((columns, levels, rows), jnp.float32),
        in_specs=[block, block, block]
        + [whole(value) for value in (ctrl, stencil, band, row_loc, level_loc)],
        out_specs=pl.BlockSpec((columns, levels, rows), lambda k: (0, 0, 0)),
        scratch_shapes=[
            pltpu.VMEM((window, levels, rows), jnp.bfloat16),
            pltpu.VMEM((columns, levels, rows), jnp.bfloat16),
            pltpu.VMEM((columns, levels, rows), jnp.bfloat16),
            pltpu.VMEM((columns * levels, rows), jnp.bfloat16),
        ],
        compiler_params=pltpu.CompilerParams(
            dimension_semantics=("arbitrary",), vmem_limit_bytes=24 * 1024 * 1024
        ),
        cost_estimate=pl.CostEstimate(
            flops=4 * flops, bytes_accessed=6 * own.size, transcendentals=0
        ),
    )(before, own, after, ctrl, stencil, band, row_loc, level_loc)


def neighbours(value):
    peers = lax.axis_size("tile")
    up = [(i, (i + 1) % peers) for i in range(peers - 1)]
    down = [(j, i) for i, j in up]
    return lax.ppermute(value, "tile", up), lax.ppermute(value, "tile", down)


def fused_increment(
    ens_coarse, col_interp, row_weights, ctrl_vec, band_loc, row_loc, level_loc, total_members
):
    fine_rows = row_weights.shape[1]
    stencil = row_matrix(row_weights, fine_rows, fine_rows // 2).T
    band = jnp.kron(band_loc, jnp.eye(GROUP, dtype=jnp.bfloat16))
    ctrl_own = jnp.swapaxes(ctrl_vec[0], 0, 1)
    ctrl_before, ctrl_after = neighbours(ctrl_own)
    ctrl = jnp.concatenate([ctrl_before, ctrl_own, ctrl_after], axis=0)
    members = ens_coarse.shape[1]
    chunks = CHUNKS if members % CHUNKS == 0 else 1
    size = members // chunks
    total = None
    for chunk in range(chunks):
        piece = ens_coarse[0, chunk * size : (chunk + 1) * size]
        coarse_cols = jnp.einsum(
            "klic,jc->jkil", piece, col_interp, preferred_element_type=jnp.float32
        ).astype(jnp.bfloat16)
        peers = lax.axis_size("tile")
        columns = coarse_cols.shape[0] // peers
        blocks = coarse_cols.reshape((peers, columns) + coarse_cols.shape[1:])
        moved = lax.all_to_all(blocks, "tile", split_axis=0, concat_axis=0, tiled=True)
        own = jnp.transpose(moved, (2, 1, 0, 3, 4))
        own = own.reshape(size, columns, -1, own.shape[-1])
        before, after = neighbours(own)
        part = member_sum(before, own, after, ctrl, stencil, band, row_loc, level_loc)
        total = part if total is None else total + part
    return swap_add(jnp.swapaxes(total, 0, 1)) / (total_members - 1)


def body(
    ens_coarse,
    col_interp,
    row_weights,
    ctrl_vec,
    band_loc,
    row_loc,
    level_loc,
    hx_pert,
    innov,
    obs_prec,
    obs_region,
):
    total_members = hx_pert.shape[1]
    observed = hx_pert[0]
    weighted = (observed * obs_prec[0][None, :]).astype(jnp.bfloat16)
    labels = lax.broadcasted_iota(jnp.int32, (NREG, observed.shape[1]), 0)
    member_of = obs_region[0][None, :] == labels
    masked = jnp.where(member_of[:, None, :], weighted[None], jnp.zeros((), jnp.bfloat16))
    gram_sums = jnp.einsum("rko,jo->rkj", masked, observed, preferred_element_type=jnp.float32)
    innov_rows = jnp.where(member_of, innov[0][None, :], 0.0)
    right_side = jnp.dot(
        innov_rows, weighted.astype(jnp.float32).T, precision=lax.Precision.HIGHEST
    )
    sums = jnp.concatenate([gram_sums, right_side[:, :, None]], axis=2)
    sums = swap_add(lax.psum(sums, "grp") if lax.axis_size("grp") > 1 else sums)
    plan = fused_increment if lax.axis_size("grp") == 1 else plain_increment
    increment = plan(
        ens_coarse, col_interp, row_weights, ctrl_vec, band_loc, row_loc, level_loc, total_members
    )
    own_weights = solve_weights(sums[:, :, :total_members], sums[:, :, total_members])
    weights = collect(own_weights)
    return (increment[None], weights)


def solution(mesh):
    placed = (
        P("grp", "mem", None, "tile", None),
        P(),
        P(),
        P("grp", None, "tile", None),
        P("tile", None),
        P(),
        P(),
        P("grp", None, ("tile", "mem")),
        P("grp", ("tile", "mem")),
        P("grp", ("tile", "mem")),
        P("grp", ("tile", "mem")),
    )
    return jax.shard_map(
        body,
        mesh=mesh,
        in_specs=placed,
        out_specs=(P("grp", "mem", "tile", None), P("tile", None)),
        check_vma=False,
    )
```
